32 devices in a mesh: dp: 8 (over z, y), expert: 2 (over core), tensor: 2 (over x).
Axes of the slice: x: 2, y: 2, z: 4, core: 2. Of those that a mesh axis runs over, the one named last changes fastest.
Arguments:
- dense_act: bfloat16 [2, 32, 512, 3584], P(None, 'dp', 'expert', 'tensor'), may hold values from -6 to 6
- dense_cot: bfloat16 [2, 32, 512, 3584], P(None, 'dp', ('expert', 'tensor')), may hold values from -6 to 6
- dense_proj_in: bfloat16 [2, 3584, 128], P(None, 'tensor'), may hold values from -0.09375 to 0.09375
- dense_proj_out: bfloat16 [2, 3584, 128], replicated, may hold values from -0.09375 to 0.09375
- expert_act: bfloat16 [32, 8, 64, 2560], P('dp', 'expert', None, 'tensor'), may hold values from -6 to 6
- expert_cot: bfloat16 [32, 8, 64, 3584], P('dp', 'expert', 'tensor'), may hold values from -6 to 6
- expert_proj_in: bfloat16 [2560, 128], P('tensor'), may hold values from -0.125 to 0.125
- expert_proj_out: bfloat16 [3584, 128], replicated, may hold values from -0.09375 to 0.09375
- dense_valid: float32 [2, 128, 128], replicated, may hold values from -0.0012207031 to 0.0012207031
- expert_valid: float32 [8, 128, 128], P('expert'), may hold values from -0.0012207031 to 0.0012207031
- domain_ids: int32 [32], P('dp'), may hold values from 0 to 63
- prior_mix: float32 [64], replicated, may hold values from 0.002 to 0.05
Outputs:
- log_mixture_weights: float32 [64], P('dp')
The draws below stay inside these ranges and needn't reach their ends.
All inputs are finite; a program needn't handle non-finite values.
Results may differ from the reference program's by a relative error of at most 0.0003.
Values sent between devices are 32-bit elements; how exact they have to be, the bound alone decides.
A program may use at most 128 MiB of HBM per device.

```python
import math
import jax
import jax.numpy as jnp
from jax import lax

D = 3584
FFE = 2560
R = 128
LAYERS = 2
DOMAINS = 64
TOK_MB = 512
CAP = 64
MICRO = 32
EXPERTS = 8


def plant(array, own_key, low, high):
    place = [jax.random.randint(jax.random.fold_in(own_key, axis), (), 0, length) for axis, length in enumerate(array.shape)]
    main_axis = array.shape.index(max(array.shape))
    neighbour = place[:main_axis] + [(place[main_axis] + 1) % array.shape[main_axis]] + place[main_axis + 1:]
    return array.at[tuple(place)].set(low).at[tuple(neighbour)].set(high)


def steps_of(own_key, extent, cuts, smallest, high):
    def one(position, shards_of):
        heights = jax.random.uniform(jax.random.fold_in(jax.random.fold_in(own_key, 6), position), (shards_of,), jnp.float32, smallest / len(cuts), high / len(cuts))
        return jnp.repeat(jnp.exp(heights), extent[position] // shards_of).reshape((-1,) + (1,) * (len(extent) - position - 1))

    loudness = one(*cuts[0])
    for cut in cuts[1:]:
        loudness = loudness * one(*cut)
    return loudness


def gaussian(key, shape, scale, reach, split=(), kind=jnp.bfloat16):
    entries = jax.random.normal(key, shape, jnp.float32) * scale
    if len(split) > 0:
        entries = steps_of(key, shape, split, -0.22, 0.18) * entries
    return jnp.clip(entries, min=-reach, max=reach).astype(kind)


def setup_inputs(seed: int = 0) -> dict:
    key_list = jax.random.split(jax.random.key(seed), 13)
    dense_act = gaussian(key_list[0], (LAYERS, MICRO, TOK_MB, D), 1.0, 6.0, ((1, 8), (2, 2), (3, 2)))
    dense_cot = gaussian(key_list[1], (LAYERS, MICRO, TOK_MB, D), 1.0, 6.0, ((1, 8), (2, 4)))
    dense_proj_in = gaussian(key_list[2], (LAYERS, D, R), D ** -0.5, 0.09375, ((1, 2),))
    dense_proj_out = gaussian(key_list[3], (LAYERS, D, R), D ** -0.5, 0.09375)
    expert_act = gaussian(key_list[4], (MICRO, EXPERTS, CAP, FFE), 1.0, 6.0, ((0, 8), (1, 2), (3, 2)))
    expert_cot = gaussian(key_list[5], (MICRO, EXPERTS, CAP, D), 1.0, 6.0, ((0, 8), (1, 2), (2, 2)))
    expert_proj_in = gaussian(key_list[6], (FFE, R), FFE ** -0.5, 0.125, ((0, 2),))
    expert_proj_out = gaussian(key_list[7], (D, R), D ** -0.5, 0.09375)
    dense_valid = gaussian(key_list[8], (LAYERS, R, R), (R * R * (LAYERS * TOK_MB + EXPERTS * CAP)) ** -0.5, 0.0012207031, (), jnp.float32)
    expert_valid = gaussian(key_list[9], (EXPERTS, R, R), (R * R * (LAYERS * TOK_MB + EXPERTS * CAP)) ** -0.5, 0.0012207031, ((0, 2),), jnp.float32)
    domain_ids = plant(jax.random.randint(key_list[10], (MICRO,), 0, DOMAINS), jax.random.fold_in(key_list[10], 1), 0, DOMAINS - 1).astype(jnp.int32)
    prior_mix = jnp.clip(jnp.exp(jax.random.uniform(key_list[11], (DOMAINS,), jnp.float32, math.log(0.002), math.log(0.05))), 0.002, 0.05)
    return dict(dense_act=dense_act, dense_cot=dense_cot, dense_proj_in=dense_proj_in, dense_proj_out=dense_proj_out, expert_act=expert_act, expert_cot=expert_cot, expert_proj_in=expert_proj_in, expert_proj_out=expert_proj_out, dense_valid=dense_valid, expert_valid=expert_valid, domain_ids=domain_ids, prior_mix=prior_mix)


def reference(dense_act, dense_cot, dense_proj_in, dense_proj_out, expert_act, expert_cot, expert_proj_in, expert_proj_out, dense_valid, expert_valid, domain_ids, prior_mix):
    width = dense_act.shape[3]
    micro = dense_act.shape[1]
    tokens = dense_act.shape[2]
    rank = dense_proj_in.shape[2]
    score = jnp.zeros((micro,), jnp.float32)
    for layer in range(dense_act.shape[0]):
        dense_update_vector = jnp.dot(dense_act[layer].reshape(-1, width), dense_proj_in[layer], preferred_element_type=jnp.float32).reshape(micro, tokens, rank)
        dense_weight_matrix = jnp.dot(dense_cot[layer].reshape(-1, width), dense_proj_out[layer], preferred_element_type=jnp.float32).reshape(micro, tokens, rank)
        sketch = jnp.einsum('mtr,mts->mrs', dense_update_vector, dense_weight_matrix, precision=lax.Precision.HIGHEST)
        score = score + lax.optimization_barrier(jnp.sum(sketch * dense_valid[layer][None], axis=(1, 2)))
    experts = expert_act.shape[1]
    slots = expert_act.shape[2]
    expert_u = jnp.dot(expert_act.reshape(-1, expert_act.shape[3]), expert_proj_in, preferred_element_type=jnp.float32).reshape(micro, experts, slots, rank)
    expert_weight_matrix = jnp.dot(expert_cot.reshape(-1, width), expert_proj_out, preferred_element_type=jnp.float32).reshape(micro, experts, slots, rank)
    expert_sketch = jnp.einsum('mecr,mecs->mers', expert_u, expert_weight_matrix, precision=lax.Precision.HIGHEST)
    score = score + lax.optimization_barrier(jnp.sum(expert_sketch * expert_valid[None], axis=(1, 2, 3)))
    domains = prior_mix.shape[0]
    onehot = (domain_ids[:, None] == jnp.arange(domains, dtype=jnp.int32)[None, :]).astype(jnp.float32)
    domain_total = jnp.dot(score, onehot, precision=lax.Precision.HIGHEST)
    spread = jnp.sqrt(jnp.mean(domain_total * domain_total) + 1e-06)
    z_value = domain_total / spread
    mass = jnp.sum(prior_mix * jnp.exp(0.5 * z_value))
    return jnp.log(prior_mix) + 0.5 * z_value - jnp.log(mass)
```

```python
import functools

import jax
import jax.numpy as jnp
from jax import lax
from jax.experimental import pallas as pl
from jax.experimental.pallas import tpu as pltpu
from jax.sharding import PartitionSpec as P

MESH = pl.DeviceIdType.MESH
HIGHEST = lax.Precision.HIGHEST


def kernel(
    sizes,
    act, cot, pin, pout, eact, ecot, epin, epout, dval, evals, ids, prior,
    out,
    va, vc, vpin, vpout, vea, vec, vepin, vepout, vdv, vev, vids, vprior,
    dsend, drecv, esend, erecv, dg, eg, acc, rows,
    a_sem, c_sem, ea_sem, ec_sem, w_sem,
    ds_sem, dr_sem, es_sem, er_sem, row_send, row_recv,
):
    nd, ne, nt = sizes
    n = nd * ne * nt
    dp, ex, tx = lax.axis_index("dp"), lax.axis_index("expert"), lax.axis_index("tensor")
    me = (dp * ne + ex) * nt + tx
    layers, micro, q, rank = cot.shape[0], cot.shape[1], cot.shape[2], pin.shape[2]
    experts, qc = ecot.shape[1], ecot.shape[2]
    hidden = eact.shape[3]
    dim = ecot.shape[3]

    def split(k):
        return lax.div(k, micro), lax.rem(k, micro)

    def load_a(o, l, m):
        first = pl.multiple_of(lax.rem(tx + o, nt) * q, q)
        return pltpu.make_async_copy(act.at[l, m, pl.ds(first, q), :], va.at[o, l, m], a_sem.at[o, l, m])

    def load_ea(o, m):
        first = pl.multiple_of(lax.rem(tx + o, nt) * qc, qc)
        return pltpu.make_async_copy(eact.at[m, :, pl.ds(first, qc), :], vea.at[o, m], ea_sem.at[o, m])

    def load_c(l, m):
        return pltpu.make_async_copy(cot.at[l, m], vc.at[l, m], c_sem.at[l, m])

    def load_ec(m):
        return pltpu.make_async_copy(ecot.at[m], vec.at[m], ec_sem.at[m])

    weights = [
        pltpu.make_async_copy(src, dst, w_sem.at[i])
        for i, (src, dst) in enumerate(
            [(epin, vepin), (pin, vpin), (pout, vpout), (dval, vdv), (epout, vepout), (evals, vev), (ids, vids), (prior, vprior)]
        )
    ]
    w_epin, w_pin, w_pout, w_dval, w_epout, w_eval, w_ids, w_prior = weights

    def send_d(o, l, m):
        return pltpu.make_async_remote_copy(
            src_ref=dsend.at[o - 1, l, m], dst_ref=drecv.at[o - 1, l, m],
            send_sem=ds_sem.at[o - 1, l, m], recv_sem=dr_sem.at[o - 1, l, m],
            device_id={"dp": dp, "expert": ex, "tensor": lax.rem(tx + o, nt)}, device_id_type=MESH,
        )

    def send_e(o, m):
        return pltpu.make_async_remote_copy(
            src_ref=esend.at[o - 1, m], dst_ref=erecv.at[o - 1, m],
            send_sem=es_sem.at[o - 1, m], recv_sem=er_sem.at[o - 1, m],
            device_id={"dp": dp, "expert": ex, "tensor": lax.rem(tx + o, nt)}, device_id_type=MESH,
        )

    def peer(i):
        t = lax.rem(me + i, n)
        return {"dp": lax.div(t, ne * nt), "expert": lax.rem(lax.div(t, nt), ne), "tensor": lax.rem(t, nt)}

    w_epin.start()
    for o in range(1, nt):
        load_ea(o, 0).start()
    for m in range(1, micro):
        for o in range(1, nt):
            load_ea(o, m).start()
    w_pin.start()

    barrier = pltpu.get_barrier_semaphore()

    @pl.loop(1, n)
    def _(i):
        pl.semaphore_signal(barrier, inc=1, device_id=peer(i), device_id_type=MESH)

    acc[...] = jnp.zeros_like(acc)
    w_epin.wait()

    def expert_out(m):
        for o in range(1, nt):
            load_ea(o, m).wait()
            esend[o - 1, m] = jnp.dot(
                vea[o, m].reshape(experts * qc, hidden), vepin[...], preferred_element_type=jnp.float32
            )
        for l in range(layers):
            for o in range(1, nt):
                load_a(o, l, m).start()

    expert_out(0)
    pl.semaphore_wait(barrier, n - 1)
    for o in range(1, nt):
        send_e(o, 0).start()

    @pl.loop(1, micro)
    def _(m):
        expert_out(m)
        for o in range(1, nt):
            send_e(o, m).start()

    w_pout.start()
    w_dval.start()
    w_pin.wait()

    @pl.loop(0, layers * micro)
    def _(k):
        l, m = split(k)
        for o in range(1, nt):
            load_a(o, l, m).wait()
            dsend[o - 1, l, m] = jnp.dot(va[o, l, m], vpin[l], preferred_element_type=jnp.float32)
        load_a(0, l, m).start()
        load_c(l, m).start()
        for o in range(1, nt):
            send_d(o, l, m).start()

    w_epout.start()
    w_eval.start()
    for m in range(micro):
        load_ea(0, m).start()
        load_ec(m).start()
    w_ids.start()
    w_prior.start()
    w_pout.wait()
    w_dval.wait()

    def fold(m, value):
        acc[m] += jnp.sum(value.reshape(-1, 8, rank), axis=0)

    @pl.loop(0, layers * micro)
    def _(k):
        l, m = split(k)
        load_a(0, l, m).wait()
        load_c(l, m).wait()
        u = jnp.dot(va[0, l, m], vpin[l], preferred_element_type=jnp.float32)
        w = jnp.dot(vc[l, m], vpout[l], preferred_element_type=jnp.float32)
        g = lax.dot_general(
            w, vdv[l], (((1,), (1,)), ((), ())), precision=HIGHEST, preferred_element_type=jnp.float32
        )
        dg[l, m] = g
        fold(m, u * g)

    w_epout.wait()
    w_eval.wait()

    @pl.loop(0, micro)
    def _(m):
        load_ea(0, m).wait()
        load_ec(m).wait()
        u = jnp.dot(vea[0, m].reshape(experts * qc, hidden), vepin[...], preferred_element_type=jnp.float32)
        w = jnp.dot(vec[m].reshape(experts * qc, dim), vepout[...], preferred_element_type=jnp.float32)
        g = jnp.concatenate(
            [
                lax.dot_general(
                    w[e * qc : (e + 1) * qc], vev[e], (((1,), (1,)), ((), ())),
                    precision=HIGHEST, preferred_element_type=jnp.float32,
                )
                for e in range(experts)
            ],
            axis=0,
        )
        eg[m] = g
        fold(m, u * g)

    @pl.loop(0, micro)
    def _(m):
        for o in range(1, nt):
            send_e(o, m).wait()
            fold(m, erecv[o - 1, m] * eg[m])

    w_ids.wait()
    w_prior.wait()

    @pl.loop(0, layers * micro)
    def _(k):
        l, m = split(k)
        for o in range(1, nt):
            send_d(o, l, m).wait()
            fold(m, drecv[o - 1, l, m] * dg[l, m])

    lanes = rows.shape[2]
    lane = lax.broadcasted_iota(jnp.int32, (1, lanes), 1)
    part = jnp.zeros((1, lanes), jnp.float32)
    for m in range(micro):
        score = jnp.sum(jnp.sum(acc[m], axis=0, keepdims=True), axis=1, keepdims=True)
        part = part + jnp.where(lane == vids[m], score, 0.0)
    rows[me] = part

    def send_row(i):
        return pltpu.make_async_remote_copy(
            src_ref=rows.at[me], dst_ref=rows.at[me], send_sem=row_send, recv_sem=row_recv,
            device_id=peer(i), device_id_type=MESH,
        )

    @pl.loop(1, n)
    def _(i):
        send_row(i).start()

    others = rows.at[pl.ds(0, n - 1)]
    pltpu.make_async_copy(others, others, row_recv).wait()
    domains = prior.shape[1]
    total = jnp.sum(rows[...], axis=0)[:, :domains]
    spread = jnp.sqrt(jnp.sum(total * total, axis=1, keepdims=True) * (1.0 / domains) + 1e-06)
    z = total / spread
    mix = vprior[...]
    mass = jnp.sum(mix * jnp.exp(0.5 * z), axis=1, keepdims=True)
    out[...] = jnp.log(mix) + 0.5 * z - jnp.log(mass)
    pltpu.make_async_copy(others, others, row_send).wait()


def per_device(sizes, *args):
    (act, cot, pin, pout, eact, ecot, epin, epout, dval, evals, ids, prior) = args
    nd, ne, nt = sizes
    n = nd * ne * nt
    layers, micro, q, dim = cot.shape
    rank, feat = pin.shape[2], pin.shape[1]
    experts, qc, hidden = ecot.shape[1], ecot.shape[2], eact.shape[3]
    domains = prior.shape[0]
    lanes = -(-domains // 128) * 128
    bf, f32 = jnp.bfloat16, jnp.float32
    V, dma = pltpu.VMEM, pltpu.SemaphoreType.DMA
    logs = pl.pallas_call(
        functools.partial(kernel, sizes),
        out_shape=jax.ShapeDtypeStruct((1, domains), f32),
        in_specs=[pl.BlockSpec(memory_space=pl.ANY)] * 12,
        out_specs=pl.BlockSpec(memory_space=pltpu.VMEM),
        scratch_shapes=[
            V((nt, layers, micro, q, feat), bf),
            V((layers, micro, q, dim), bf),
            V(pin.shape, bf),
            V(pout.shape, bf),
            V((nt, micro, experts, qc, hidden), bf),
            V((micro, experts, qc, dim), bf),
            V(epin.shape, bf),
            V(epout.shape, bf),
            V(dval.shape, f32),
            V(evals.shape, f32),
            pltpu.SMEM(ids.shape, jnp.int32),
            V((1, domains), f32),
            V((nt - 1, layers, micro, q, rank), f32),
            V((nt - 1, layers, micro, q, rank), f32),
            V((nt - 1, micro, experts * qc, rank), f32),
            V((nt - 1, micro, experts * qc, rank), f32),
            V((layers, micro, q, rank), f32),
            V((micro, experts * qc, rank), f32),
            V((micro, 8, rank), f32),
            V((n, 1, lanes), f32),
            dma((nt, layers, micro)),
            dma((layers, micro)),
            dma((nt, micro)),
            dma((micro,)),
            dma((8,)),
            dma((nt - 1, layers, micro)),
            dma((nt - 1, layers, micro)),
            dma((nt - 1, micro)),
            dma((nt - 1, micro)),
            dma,
            dma,
        ],
        compiler_params=pltpu.CompilerParams(
            collective_id=0, has_side_effects=True, vmem_limit_bytes=60 * 1024 * 1024
        ),
        name="align",
    )(act, cot, pin, pout, eact, ecot, epin, epout, dval, evals, ids, prior.reshape(1, domains))
    share = domains // nd
    return lax.dynamic_slice_in_dim(logs[0], lax.axis_index("dp") * share, share, 0)


def solution(mesh):
    sizes = (mesh.shape["dp"], mesh.shape["expert"], mesh.shape["tensor"])
    placed = (
        P(None, "dp", "expert", "tensor"),
        P(None, "dp", ("expert", "tensor"), None),
        P(None, "tensor", None),
        P(),
        P("dp", "expert", None, "tensor"),
        P("dp", "expert", "tensor", None),
        P("tensor", None),
        P(),
        P(),
        P("expert", None, None),
        P("dp"),
        P(),
    )
    return jax.shard_map(
        functools.partial(per_device, sizes), mesh=mesh, in_specs=placed, out_specs=P("dp"), check_vma=False
    )
```

```python
import functools

import jax
import jax.numpy as jnp
from jax import lax
from jax.experimental import pallas as pl
from jax.experimental.pallas import tpu as pltpu
from jax.sharding import PartitionSpec as P

MESH = pl.DeviceIdType.MESH
HIGHEST = lax.Precision.HIGHEST


def kernel(
    sizes,
    act, cot, pin, pout, eact, ecot, epin, epout, dval, evals, ids, prior,
    out,
    va, vc, vpin, vpout, vea, vec, vepin, vepout, vdv, vev, vids, vprior,
    dsend, drecv, esend, erecv, dg, eg, acc, rows,
    a_sem, c_sem, ea_sem, ec_sem, w_sem,
    ds_sem, dr_sem, es_sem, er_sem, row_send, row_recv,
):
    nd, ne, nt = sizes
    n = nd * ne * nt
    dp, ex, tx = lax.axis_index("dp"), lax.axis_index("expert"), lax.axis_index("tensor")
    me = (dp * ne + ex) * nt + tx
    layers, micro, q, rank = cot.shape[0], cot.shape[1], cot.shape[2], pin.shape[2]
    experts, qc = ecot.shape[1], ecot.shape[2]
    hidden = eact.shape[3]
    dim = ecot.shape[3]

    def split(k):
        return lax.div(k, micro), lax.rem(k, micro)

    def load_a(o, l, m):
        first = pl.multiple_of(lax.rem(tx + o, nt) * q, q)
        return pltpu.make_async_copy(act.at[l, m, pl.ds(first, q), :], va.at[o, l, m], a_sem.at[o, l, m])

    def load_ea(o, m):
        first = pl.multiple_of(lax.rem(tx + o, nt) * qc, qc)
        return pltpu.make_async_copy(eact.at[m, :, pl.ds(first, qc), :], vea.at[o, m], ea_sem.at[o, m])

    def load_c(l, m):
        return pltpu.make_async_copy(cot.at[l, m], vc.at[l, m], c_sem.at[l, m])

    def load_ec(m):
        return pltpu.make_async_copy(ecot.at[m], vec.at[m], ec_sem.at[m])

    weights = [
        pltpu.make_async_copy(src, dst, w_sem.at[i])
        for i, (src, dst) in enumerate(
            [(epin, vepin), (pin, vpin), (pout, vpout), (dval, vdv), (epout, vepout), (evals, vev), (ids, vids), (prior, vprior)]
        )
    ]
    w_epin, w_pin, w_pout, w_dval, w_epout, w_eval, w_ids, w_prior = weights

    def send_d(o, l, m):
        return pltpu.make_async_remote_copy(
            src_ref=dsend.at[o - 1, l, m], dst_ref=drecv.at[o - 1, l, m],
            send_sem=ds_sem.at[o - 1, l, m], recv_sem=dr_sem.at[o - 1, l, m],
            device_id={"dp": dp, "expert": ex, "tensor": lax.rem(tx + o, nt)}, device_id_type=MESH,
        )

    def send_e(o, m):
        return pltpu.make_async_remote_copy(
            src_ref=esend.at[o - 1, m], dst_ref=erecv.at[o - 1, m],
            send_sem=es_sem.at[o - 1, m], recv_sem=er_sem.at[o - 1, m],
            device_id={"dp": dp, "expert": ex, "tensor": lax.rem(tx + o, nt)}, device_id_type=MESH,
        )

    def peer(i):
        t = lax.rem(me + i, n)
        return {"dp": lax.div(t, ne * nt), "expert": lax.rem(lax.div(t, nt), ne), "tensor": lax.rem(t, nt)}

    barrier = pltpu.get_barrier_semaphore()

    @pl.loop(1, n)
    def _(i):
        pl.semaphore_signal(barrier, inc=1, device_id=peer(i), device_id_type=MESH)

    w_epin.start()
    for o in range(1, nt):
        load_ea(o, 0).start()
    for m in range(1, micro):
        for o in range(1, nt):
            load_ea(o, m).start()
    w_pin.start()

    acc[...] = jnp.zeros_like(acc)
    w_epin.wait()

    def expert_out(m):
        for o in range(1, nt):
            load_ea(o, m).wait()
            esend[o - 1, m] = jnp.dot(
                vea[o, m].reshape(experts * qc, hidden), vepin[...], preferred_element_type=jnp.float32
            )
        for l in range(layers):
            for o in range(1, nt):
                load_a(o, l, m).start()

    expert_out(0)
    pl.semaphore_wait(barrier, n - 1)
    for o in range(1, nt):
        send_e(o, 0).start()

    @pl.loop(1, micro)
    def _(m):
        expert_out(m)
        for o in range(1, nt):
            send_e(o, m).start()

    w_pout.start()
    w_dval.start()
    w_pin.wait()

    @pl.loop(0, layers * micro)
    def _(k):
        l, m = split(k)
        for o in range(1, nt):
            load_a(o, l, m).wait()
            dsend[o - 1, l, m] = jnp.dot(va[o, l, m], vpin[l], preferred_element_type=jnp.float32)
        load_a(0, l, m).start()
        load_c(l, m).start()
        for o in range(1, nt):
            send_d(o, l, m).start()

    w_epout.start()
    w_eval.start()
    for m in range(micro):
        load_ea(0, m).start()
        load_ec(m).start()
    w_ids.start()
    w_prior.start()
    w_pout.wait()
    w_dval.wait()

    def fold(m, value):
        acc[m] += jnp.sum(value.reshape(-1, 8, rank), axis=0)

    @pl.loop(0, layers * micro)
    def _(k):
        l, m = split(k)
        load_a(0, l, m).wait()
        load_c(l, m).wait()
        u = jnp.dot(va[0, l, m], vpin[l], preferred_element_type=jnp.float32)
        w = jnp.dot(vc[l, m], vpout[l], preferred_element_type=jnp.float32)
        g = lax.dot_general(
            w, vdv[l], (((1,), (1,)), ((), ())), precision=HIGHEST, preferred_element_type=jnp.float32
        )
        dg[l, m] = g
        fold(m, u * g)

    w_epout.wait()
    w_eval.wait()

    @pl.loop(0, micro)
    def _(m):
        load_ea(0, m).wait()
        load_ec(m).wait()
        u = jnp.dot(vea[0, m].reshape(experts * qc, hidden), vepin[...], preferred_element_type=jnp.float32)
        w = jnp.dot(vec[m].reshape(experts * qc, dim), vepout[...], preferred_element_type=jnp.float32)
        g = jnp.concatenate(
            [
                lax.dot_general(
                    w[e * qc : (e + 1) * qc], vev[e], (((1,), (1,)), ((), ())),
                    precision=HIGHEST, preferred_element_type=jnp.float32,
                )
                for e in range(experts)
            ],
            axis=0,
        )
        eg[m] = g
        fold(m, u * g)

    @pl.loop(0, micro)
    def _(m):
        for o in range(1, nt):
            send_e(o, m).wait()
            fold(m, erecv[o - 1, m] * eg[m])

    w_ids.wait()
    w_prior.wait()

    @pl.loop(0, layers * micro)
    def _(k):
        l, m = split(k)
        for o in range(1, nt):
            send_d(o, l, m).wait()
            fold(m, drecv[o - 1, l, m] * dg[l, m])

    lanes = rows.shape[2]
    lane = lax.broadcasted_iota(jnp.int32, (1, lanes), 1)
    part = jnp.zeros((1, lanes), jnp.float32)
    for m in range(micro):
        score = jnp.sum(jnp.sum(acc[m], axis=0, keepdims=True), axis=1, keepdims=True)
        part = part + jnp.where(lane == vids[m], score, 0.0)
    rows[me] = part

    def send_row(i):
        return pltpu.make_async_remote_copy(
            src_ref=rows.at[me], dst_ref=rows.at[me], send_sem=row_send, recv_sem=row_recv,
            device_id=peer(i), device_id_type=MESH,
        )

    @pl.loop(1, n)
    def _(i):
        send_row(i).start()

    others = rows.at[pl.ds(0, n - 1)]
    pltpu.make_async_copy(others, others, row_recv).wait()
    domains = prior.shape[1]
    total = jnp.sum(rows[...], axis=0)[:, :domains]
    spread = jnp.sqrt(jnp.sum(total * total, axis=1, keepdims=True) * (1.0 / domains) + 1e-06)
    z = total / spread
    mix = vprior[...]
    mass = jnp.sum(mix * jnp.exp(0.5 * z), axis=1, keepdims=True)
    out[...] = jnp.log(mix) + 0.5 * z - jnp.log(mass)
    pltpu.make_async_copy(others, others, row_send).wait()


def per_device(sizes, *args):
    (act, cot, pin, pout, eact, ecot, epin, epout, dval, evals, ids, prior) = args
    nd, ne, nt = sizes
    n = nd * ne * nt
    layers, micro, q, dim = cot.shape
    rank, feat = pin.shape[2], pin.shape[1]
    experts, qc, hidden = ecot.shape[1], ecot.shape[2], eact.shape[3]
    domains = prior.shape[0]
    lanes = -(-domains // 128) * 128
    bf, f32 = jnp.bfloat16, jnp.float32
    V, dma = pltpu.VMEM, pltpu.SemaphoreType.DMA
    logs = pl.pallas_call(
        functools.partial(kernel, sizes),
        out_shape=jax.ShapeDtypeStruct((1, domains), f32),
        in_specs=[pl.BlockSpec(memory_space=pl.ANY)] * 12,
        out_specs=pl.BlockSpec(memory_space=pltpu.VMEM),
        scratch_shapes=[
            V((nt, layers, micro, q, feat), bf),
            V((layers, micro, q, dim), bf),
            V(pin.shape, bf),
            V(pout.shape, bf),
            V((nt, micro, experts, qc, hidden), bf),
            V((micro, experts, qc, dim), bf),
            V(epin.shape, bf),
            V(epout.shape, bf),
            V(dval.shape, f32),
            V(evals.shape, f32),
            pltpu.SMEM(ids.shape, jnp.int32),
            V((1, domains), f32),
            V((nt - 1, layers, micro, q, rank), f32),
            V((nt - 1, layers, micro, q, rank), f32),
            V((nt - 1, micro, experts * qc, rank), f32),
            V((nt - 1, micro, experts * qc, rank), f32),
            V((layers, micro, q, rank), f32),
            V((micro, experts * qc, rank), f32),
            V((micro, 8, rank), f32),
            V((n, 1, lanes), f32),
            dma((nt, layers, micro)),
            dma((layers, micro)),
            dma((nt, micro)),
            dma((micro,)),
            dma((8,)),
            dma((nt - 1, layers, micro)),
            dma((nt - 1, layers, micro)),
            dma((nt - 1, micro)),
            dma((nt - 1, micro)),
            dma,
            dma,
        ],
        compiler_params=pltpu.CompilerParams(
            collective_id=0, has_side_effects=True, vmem_limit_bytes=60 * 1024 * 1024
        ),
        name="align",
    )(act, cot, pin, pout, eact, ecot, epin, epout, dval, evals, ids, prior.reshape(1, domains))
    share = domains // nd
    return lax.dynamic_slice_in_dim(logs[0], lax.axis_index("dp") * share, share, 0)


def solution(mesh):
    sizes = (mesh.shape["dp"], mesh.shape["expert"], mesh.shape["tensor"])
    placed = (
        P(None, "dp", "expert", "tensor"),
        P(None, "dp", ("expert", "tensor"), None),
        P(None, "tensor", None),
        P(),
        P("dp", "expert", None, "tensor"),
        P("dp", "expert", "tensor", None),
        P("tensor", None),
        P(),
        P(),
        P("expert", None, None),
        P("dp"),
        P(),
    )
    return jax.shard_map(
        functools.partial(per_device, sizes), mesh=mesh, in_specs=placed, out_specs=P("dp"), check_vma=False
    )
```
